1024 devices in a mesh: prow: 16 (over y, x_lo), pcol: 64 (over z, x_hi, core).
Axes of the slice: x: 8 (x_hi: 4, x_lo: 2; x = x_hi * 2 + x_lo), y: 8, z: 8, core: 2. Of those that a mesh axis runs over, the one named last changes fastest.
Arguments:
- matrix: float32 [16384, 16384], P('prow', 'pcol'), may hold values from -6 to 6
- l_panels: float32 [2, 16384, 256], P(None, ('prow', 'pcol')), may hold values from -0.375 to 0.375
- l_inverse: float32 [2, 256, 256], replicated, as said below
- pivots: int32 [2, 256], replicated, may hold values from 0 to 16383, as said below
Outputs:
- updated: float32 [16384, 16384], P('prow', 'pcol')
The draws below stay inside these ranges and needn't reach their ends.
Inputs may be any that keep to these rules, and one draw needn't show every extreme that they name: `pivots`: for each step s, entry k is either s * 256 + k or a row at or after (s + 1) * 256; the entries of one step are distinct. `l_inverse`: each block is unit lower triangular.
All inputs are finite; a program needn't handle non-finite values.
Results may differ from the reference program's by a relative error of at most 0.0001.
Values sent between devices are 32-bit elements; how exact they have to be, the bound alone decides.
A program may use at most 32 MiB of HBM per device.

```python
import jax
import jax.numpy as jnp
from jax import lax

ROWS_DEV = 1024
NB = 256
STEPS = 2
M = 16384
N = 16384


def draw_l_inverse(key, part):
    values = jax.random.normal(key, (STEPS, NB, NB))
    lower = jnp.tril(values, -1) / jnp.sqrt(jnp.float32(NB))
    return (lower + jnp.eye(NB, dtype=jnp.float32)).astype(jnp.float32)


def draw_pivots(key, part):
    row_ids = jnp.arange(M, dtype=jnp.int32)
    owners = M // ROWS_DEV
    block_last = (row_ids + 1) % ROWS_DEV == 0
    result = []
    for step in range(STEPS):
        step_key = jax.random.fold_in(key, 11 + step)
        key_level, key_rank, key_order, key_keep = jax.random.split(step_key, 4)
        level = jax.random.randint(key_level, (owners,), 0, 4)
        owner_level = jnp.repeat(level, ROWS_DEV)
        rank = jax.random.permutation(key_rank, M).astype(jnp.int32)
        score = owner_level * M + rank
        score = jnp.where(block_last, 5 * M + row_ids, score)
        score = jnp.where(row_ids < (step + 1) * NB, -1, score)
        unused, chosen = lax.top_k(score, NB)
        chosen = chosen.astype(jnp.int32)
        order = jax.random.permutation(key_order, NB).astype(jnp.int32)
        place = jnp.argmax(order == NB - 1)
        first = order[0]
        order = order.at[place].set(first).at[0].set(NB - 1)
        chosen = chosen[order]
        forced = (chosen + 1) % ROWS_DEV == 0
        keep = jax.random.randint(key_keep, (NB,), 0, 4) == 0
        keep = keep & jnp.logical_not(forced)
        if step == 0:
            keep = keep.at[0].set(True)
        own_place = step * NB + jnp.arange(NB, dtype=jnp.int32)
        result.append(jnp.where(keep, own_place, chosen))
    return jnp.stack(result).astype(jnp.int32)


def block_levels(stream_key, shape, cuts, low, top_value):
    gain = 1.0
    for position, shards_of in cuts:
        steps = jax.random.uniform(jax.random.fold_in(jax.random.fold_in(stream_key, 6), position), (shards_of,), jnp.float32, low / len(cuts), top_value / len(cuts))
        gain = gain * jnp.repeat(jnp.exp(steps), shape[position] // shards_of).reshape((-1,) + (1,) * (len(shape) - 1 - position))
    return gain


def noise(stream_key, dims, width, reach, pieces=(), kind=jnp.bfloat16):
    values = width * jax.random.normal(stream_key, dims, jnp.float32)
    if pieces:
        values = values * block_levels(stream_key, dims, pieces, -0.22, 0.18)
    return jnp.clip(values, -reach, reach).astype(kind)


def setup_inputs(seed: int = 0) -> dict:
    streams_of = jax.random.split(jax.random.key(seed), 5)
    return {
        "matrix": noise(streams_of[0], (M, N), 1.0, 6.0, ((0, 16), (1, 64)), jnp.float32),
        "l_panels": noise(streams_of[1], (STEPS, M, NB), NB ** -0.5, 0.375, ((1, 1024),), jnp.float32),
        "l_inverse": draw_l_inverse(jax.random.fold_in(streams_of[4], 71), 0),
        "pivots": draw_pivots(jax.random.fold_in(streams_of[4], 71), 0),
    }


def reference(matrix, l_panels, l_inverse, pivots):
    current = matrix
    row_ids = jnp.arange(M, dtype=jnp.int32)
    for step in range(STEPS):
        chosen = pivots[step]
        begin = step * NB
        picked = current[chosen]
        old_top = current[begin:begin + NB]
        current = current.at[chosen].set(old_top)
        upper = jnp.dot(l_inverse[step], picked, precision=lax.Precision.HIGHEST, preferred_element_type=jnp.float32)
        current = current.at[begin:begin + NB].set(upper)
        below = (row_ids >= begin + NB)[:, None]
        factor = jnp.where(below, l_panels[step], jnp.float32(0.0))
        current = current - jnp.dot(factor, upper, precision=lax.Precision.HIGHEST, preferred_element_type=jnp.float32)
    return current
```

```python
import functools

import jax
import jax.numpy as jnp
from jax import lax
from jax.experimental import pallas as pl
from jax.experimental.pallas import tpu as pltpu
from jax.sharding import PartitionSpec as P

MESH = pl.DeviceIdType.MESH
HIGHEST = lax.Precision.HIGHEST
F32 = jnp.float32
BF16 = jnp.bfloat16


def split_cols(mesh):
    cols = mesh.shape["pcol"]
    core, xh = 2, (4 if cols >= 32 else 2)
    return cols // (core * xh), xh, core


def select(onehot, values):
    high = values.astype(BF16)
    rest = values - high.astype(F32)
    mid = rest.astype(BF16)
    low = (rest - mid.astype(F32)).astype(BF16)
    out = jnp.dot(onehot, high, preferred_element_type=F32)
    out = out + jnp.dot(onehot, mid, preferred_element_type=F32)
    return out + jnp.dot(onehot, low, preferred_element_type=F32)


def matmul(a, b):
    return jnp.dot(a, b, precision=HIGHEST, preferred_element_type=F32)


def kernel(
    sizes, a_ref, lp_ref, linv_ref, piv_ref, out_ref,
    rs_src, rs_dst, x_buf, t_buf, d_top, lf, z1, base,
    rs_s, rs_r, ag_s, ag_r, sc_s, sc_r, ta_s, ta_r,
    lx_s, lx_r, lz_s, lz_r, lc_s, lc_r, own_sem,
):
    rows_n, nz, nxh, nc, nb = sizes
    chunk = nb // rows_n
    blocks = a_ref.shape[0] // nb
    me = lax.axis_index("prow")
    col = lax.axis_index("pcol")
    core = lax.rem(col, nc)
    xh = lax.rem(col // nc, nxh)
    z = col // (nc * nxh)
    first = me * a_ref.shape[0]
    is_root = me == 0

    def row_peer(d):
        return lax.rem(me + d, rows_n)

    def xh_peer(d):
        return (z * nxh + lax.rem(xh + d, nxh)) * nc + core

    def z_peer(d):
        return (lax.rem(z + d, nz) * nxh + xh) * nc + core

    partner = (z * nxh + xh) * nc + (1 - core)

    def send(src, dst, s, r, **where):
        copy = pltpu.make_async_remote_copy(
            src_ref=src, dst_ref=dst, send_sem=s, recv_sem=r,
            device_id=where, device_id_type=MESH,
        )
        return copy

    barrier = pltpu.get_barrier_semaphore()
    for d in range(1, rows_n):
        pl.semaphore_signal(barrier, inc=1, device_id={"prow": row_peer(d)}, device_id_type=MESH)
    for d in range(1, nxh):
        pl.semaphore_signal(barrier, inc=1, device_id={"pcol": xh_peer(d)}, device_id_type=MESH)
    for d in range(1, nz):
        pl.semaphore_signal(barrier, inc=1, device_id={"pcol": z_peer(d)}, device_id_type=MESH)
    pl.semaphore_signal(barrier, inc=1, device_id={"pcol": partner}, device_id_type=MESH)

    own = [
        pltpu.make_async_copy(lp_ref.at[s], lf.at[s, z * nxh + xh, core], own_sem.at[s])
        for s in range(2)
    ]
    own_t = pltpu.make_async_copy(
        a_ref.at[pl.ds(0, chunk)], t_buf.at[0, pl.ds(0, chunk)], own_sem.at[2]
    )
    for copy in own:
        copy.start()

    def as_row(s):
        return jnp.broadcast_to(piv_ref[pl.ds(s, 1), :], (nb, nb))

    row0, row1 = as_row(0), as_row(1)
    col0, col1 = row0.T, row1.T
    lane = lax.broadcasted_iota(jnp.int32, (nb, nb), 1)
    sub = lax.broadcasted_iota(jnp.int32, (nb, nb), 0)

    def source(wanted):
        hit = wanted == row0
        place = jnp.max(jnp.where(hit, lane, -1), axis=1, keepdims=True)
        place = jnp.broadcast_to(place, (nb, nb))
        return jnp.where(place >= 0, place, wanted)

    def pick(wanted):
        total = None
        for b in range(blocks):
            onehot = (wanted == lane + (first + b * nb)).astype(F32).astype(BF16)
            part = select(onehot, a_ref[pl.ds(b * nb, nb), :])
            total = part if total is None else total + part
        return total

    rs_src[0] = pick(col0).reshape(rows_n, chunk, -1)

    pl.semaphore_wait(barrier, (rows_n - 1) + (nxh - 1) + (nz - 1) + 1)

    waits = []

    lx = []
    for s in range(2):
        for d in range(1, nxh):
            copy = send(
                lp_ref.at[s], lf.at[s, z * nxh + xh, core], lx_s.at[s, d], lx_r.at[s, d],
                pcol=xh_peer(d),
            )
            copy.start()
            lx.append(copy)
    waits += lx

    def reduce_start(s):
        for d in range(1, rows_n):
            copy = send(
                rs_src.at[s, row_peer(d)], rs_dst.at[s, d], rs_s.at[s, d], rs_r.at[s, d],
                prow=row_peer(d),
            )
            copy.start()
            waits.append(copy)
        return waits[-(rows_n - 1):]

    def reduce_finish(s, copies):
        total = rs_src[s, me]
        for d in range(1, rows_n):
            copies[d - 1].wait_recv()
            total = total + rs_dst[s, d]
        mine = pl.ds(pl.multiple_of(me * chunk, chunk), chunk)
        x_buf[s, mine, :] = total

    def gather_start(buf, s, sems, r_sems):
        mine = pl.ds(pl.multiple_of(me * chunk, chunk), chunk)
        copies = []
        for d in range(1, rows_n):
            copy = send(
                buf.at[s, mine], buf.at[s, mine], sems.at[s, d], r_sems.at[s, d], prow=row_peer(d)
            )
            copy.start()
            copies.append(copy)
        waits.extend(copies)
        return copies

    def scatter_copies(src, s):
        copies = []
        for m in range(1, rows_n):
            rows = pl.ds(m * chunk, chunk)
            copies.append(
                send(src.at[rows], t_buf.at[s, rows], sc_s.at[s, m], sc_r.at[s], prow=jnp.int32(m))
            )
        return copies

    def scatter_wait(s):
        mine = pl.ds(pl.multiple_of(me * chunk, chunk), chunk)
        @pl.when(jnp.logical_not(is_root))
        def _():
            send(
                t_buf.at[s, mine], t_buf.at[s, mine], sc_s.at[s, 0], sc_r.at[s], prow=row_peer(1)
            ).wait_recv()

    rs0 = reduce_start(0)

    @pl.when(is_root)
    def _():
        own_t.start()
        for copy in scatter_copies(a_ref, 0):
            copy.start()

    z1[...] = pick(source(col1))

    @pl.when(is_root)
    def _():
        d_top[...] = pick(source(sub + nb))

    lz = [[], []]
    for s in range(2):
        own[s].wait()
        for d in range(1, nxh):
            lx[s * (nxh - 1) + d - 1].wait_recv()
        for d in range(1, nz):
            group = pl.ds(z * nxh, nxh)
            copy = send(
                lf.at[s, group, core], lf.at[s, group, core], lz_s.at[s, d], lz_r.at[s, d],
                pcol=z_peer(d),
            )
            copy.start()
            lz[s].append(copy)
    waits += lz[0] + lz[1]

    reduce_finish(0, rs0)
    ag0 = gather_start(x_buf, 0, ag_s, ag_r)

    scatter_wait(0)

    @pl.when(is_root)
    def _():
        own_t.wait()

    ta0 = gather_start(t_buf, 0, ta_s, ta_r)

    def panel_finish(s):
        for copy in lz[s]:
            copy.wait_recv()
        swap = send(
            lf.at[s, :, core], lf.at[s, :, core], lc_s.at[s], lc_r.at[s], pcol=partner
        )
        swap.start()
        swap.wait_recv()
        waits.append(swap)

    zb = nz // blocks

    def factor(s, b):
        per = nz * nxh // blocks
        return lf[s, pl.ds(b * per, per)].reshape(nb, nb)

    panel_finish(0)
    l_sel = None
    for b in range(blocks):
        onehot = (col1 == lane + (first + b * nb)).astype(F32).astype(BF16)
        part = select(onehot, factor(0, b))
        l_sel = part if l_sel is None else l_sel + part

    for copy in ag0:
        copy.wait_recv()
    upper0 = matmul(linv_ref[0], x_buf[0])
    rs_src[1] = (z1[...] - matmul(l_sel, upper0)).reshape(rows_n, chunk, -1)
    rs1 = reduce_start(1)

    @pl.when(is_root)
    def _():
        d_top[...] = d_top[...] - matmul(factor(0, 1), upper0)
        t_buf[1, pl.ds(0, chunk), :] = d_top[pl.ds(0, chunk), :]
        for copy in scatter_copies(d_top, 1):
            copy.start()

    for copy in ta0:
        copy.wait_recv()

    for b in range(blocks):
        here = sub + (first + b * nb)
        hit = (here == row0).astype(F32)
        moved = select(hit.astype(BF16), t_buf[0])
        any_hit = jnp.max(hit, axis=1, keepdims=True) > 0
        kept = jnp.where(any_hit, moved, a_ref[pl.ds(b * nb, nb), :])
        base[pl.ds(b * nb, nb), :] = kept - matmul(factor(0, b), upper0)

    reduce_finish(1, rs1)
    ag1 = gather_start(x_buf, 1, ag_s, ag_r)
    scatter_wait(1)
    ta1 = gather_start(t_buf, 1, ta_s, ta_r)

    panel_finish(1)

    for copy in ag1:
        copy.wait_recv()
    upper1 = matmul(linv_ref[1], x_buf[1])

    for copy in ta1:
        copy.wait_recv()
    for b in range(blocks):
        here = sub + (first + b * nb)
        hit = (here == row1).astype(F32)
        moved = select(hit.astype(BF16), t_buf[1])
        any_hit = jnp.max(hit, axis=1, keepdims=True) > 0
        value = jnp.where(any_hit, moved, base[pl.ds(b * nb, nb), :])
        value = value - matmul(factor(1, b), upper1)
        if b == 0:
            value = jnp.where(is_root, upper0, value)
        if b == 1:
            value = jnp.where(is_root, upper1, value)
        out_ref[pl.ds(b * nb, nb), :] = value

    for copy in waits:
        copy.wait_send()

    @pl.when(is_root)
    def _():
        for s, src in ((0, a_ref), (1, d_top)):
            for copy in scatter_copies(src, s):
                copy.wait_send()


def per_device(split, rows_n, matrix, l_panels, l_inverse, pivots):
    nz, nxh, nc = split
    rows_dev, cols_dev = matrix.shape
    nb = pivots.shape[1]
    chunk = nb // rows_n
    part = l_panels.shape[1]
    dma = pltpu.SemaphoreType.DMA
    vmem = pl.BlockSpec(memory_space=pltpu.VMEM)
    return pl.pallas_call(
        functools.partial(kernel, (rows_n, nz, nxh, nc, nb)),
        out_shape=jax.ShapeDtypeStruct(matrix.shape, F32),
        in_specs=[vmem] * 4,
        out_specs=vmem,
        scratch_shapes=[
            pltpu.VMEM((2, rows_n, chunk, cols_dev), F32),
            pltpu.VMEM((2, rows_n, chunk, cols_dev), F32),
            pltpu.VMEM((2, nb, cols_dev), F32),
            pltpu.VMEM((2, nb, cols_dev), F32),
            pltpu.VMEM((nb, cols_dev), F32),
            pltpu.VMEM((2, nz * nxh, nc, part, nb), F32),
            pltpu.VMEM((nb, cols_dev), F32),
            pltpu.VMEM((rows_dev, cols_dev), F32),
            dma((2, rows_n)), dma((2, rows_n)),
            dma((2, rows_n)), dma((2, rows_n)),
            dma((2, rows_n)), dma((2,)),
            dma((2, rows_n)), dma((2, rows_n)),
            dma((2, nxh)), dma((2, nxh)),
            dma((2, nz)), dma((2, nz)),
            dma((2,)), dma((2,)),
            dma((3,)),
        ],
        compiler_params=pltpu.CompilerParams(
            collective_id=0, has_side_effects=True, vmem_limit_bytes=48 * 1024 * 1024
        ),
    )(matrix, l_panels, l_inverse, pivots)


def solution(mesh):
    placed = (P("prow", "pcol"), P(None, ("prow", "pcol"), None), P(), P())
    body = functools.partial(per_device, split_cols(mesh), mesh.shape["prow"])
    return jax.shard_map(
        body, mesh=mesh, in_specs=placed, out_specs=P("prow", "pcol"), check_vma=False
    )
```

```python
import functools

import jax
import jax.numpy as jnp
from jax import lax
from jax.experimental import pallas as pl
from jax.experimental.pallas import tpu as pltpu
from jax.sharding import PartitionSpec as P

MESH = pl.DeviceIdType.MESH
HIGHEST = lax.Precision.HIGHEST
F32 = jnp.float32
BF16 = jnp.bfloat16


def split_cols(mesh):
    nz, core = 8, 2
    return nz, mesh.shape["pcol"] // (nz * core), core


def select(onehot, values):
    high = values.astype(BF16)
    rest = values - high.astype(F32)
    mid = rest.astype(BF16)
    low = (rest - mid.astype(F32)).astype(BF16)
    out = jnp.dot(onehot, high, preferred_element_type=F32)
    out = out + jnp.dot(onehot, mid, preferred_element_type=F32)
    return out + jnp.dot(onehot, low, preferred_element_type=F32)


def matmul(a, b):
    return jnp.dot(a, b, precision=HIGHEST, preferred_element_type=F32)


def kernel(
    sizes, a_hbm, lp_ref, linv_hbm, piv_hbm, out_ref,
    a_ref, linv_ref, piv_ref,
    rs_src, rs_dst, x_buf, t_buf, d_top, lf, z1, base,
    rs_s, rs_r, ag_s, ag_r, sc_s, sc_r, ta_s, ta_r, tf_s, tf_r,
    lx_s, lx_r, lz_s, lz_r, lc_s, lc_r, own_sem, in_sem,
):
    rows_n, nz, nxh, nc, nb = sizes
    chunk = nb // rows_n
    ny = rows_n // 2
    blocks = a_ref.shape[0] // nb
    me = lax.axis_index("prow")
    col = lax.axis_index("pcol")
    y, x = me // 2, lax.rem(me, 2)
    core = lax.rem(col, nc)
    xh = lax.rem(col // nc, nxh)
    z = col // (nc * nxh)
    first = me * a_ref.shape[0]
    is_root = me == 0

    def row_peer(d):
        return lax.rem(me + d, rows_n)

    def xh_peer(d):
        return (z * nxh + lax.rem(xh + d, nxh)) * nc + core

    def z_at(d):
        return lax.rem(z + d + nz, nz)

    def z_peer(d):
        return (z_at(d) * nxh + xh) * nc + core

    far = sorted(range(1, rows_n), key=lambda d: -min(d, rows_n - d))

    partner = (z * nxh + xh) * nc + (1 - core)

    def send(src, dst, s, r, **where):
        copy = pltpu.make_async_remote_copy(
            src_ref=src, dst_ref=dst, send_sem=s, recv_sem=r,
            device_id=where, device_id_type=MESH,
        )
        return copy

    barrier = pltpu.get_barrier_semaphore()
    for d in range(1, rows_n):
        pl.semaphore_signal(barrier, inc=1, device_id={"prow": row_peer(d)}, device_id_type=MESH)
    for d in range(1, nxh):
        pl.semaphore_signal(barrier, inc=1, device_id={"pcol": xh_peer(d)}, device_id_type=MESH)
    for d in (1, -1, 2, -2):
        pl.semaphore_signal(barrier, inc=1, device_id={"pcol": z_peer(d)}, device_id_type=MESH)
    pl.semaphore_signal(barrier, inc=1, device_id={"pcol": partner}, device_id_type=MESH)

    own = [
        pltpu.make_async_copy(lp_ref.at[s], lf.at[s, z * nxh + xh, core], own_sem.at[s])
        for s in range(2)
    ]
    own_t = pltpu.make_async_copy(a_ref.at[pl.ds(0, chunk)], t_buf.at[0, 0, 0], own_sem.at[2])
    loads = [
        pltpu.make_async_copy(src, dst, in_sem.at[n])
        for n, (src, dst) in enumerate(
            ((piv_hbm, piv_ref), (a_hbm, a_ref), (linv_hbm, linv_ref))
        )
    ]
    for copy in loads + own:
        copy.start()
    loads[0].wait()

    def as_row(s):
        return jnp.broadcast_to(piv_ref[pl.ds(s, 1), :], (nb, nb))

    row0, row1 = as_row(0), as_row(1)
    col0, col1 = row0.T, row1.T
    lane = lax.broadcasted_iota(jnp.int32, (nb, nb), 1)
    sub = lax.broadcasted_iota(jnp.int32, (nb, nb), 0)

    def source(wanted):
        hit = wanted == row0
        place = jnp.max(jnp.where(hit, lane, -1), axis=1, keepdims=True)
        place = jnp.broadcast_to(place, (nb, nb))
        return jnp.where(place >= 0, place, wanted)

    def pick(wanted):
        total = None
        for b in range(blocks):
            onehot = (wanted == lane + (first + b * nb)).astype(F32).astype(BF16)
            part = select(onehot, a_ref[pl.ds(b * nb, nb), :])
            total = part if total is None else total + part
        return total

    loads[1].wait()
    rs_src[0] = pick(col0).reshape(rows_n, chunk, -1)

    pl.semaphore_wait(barrier, (rows_n - 1) + (nxh - 1) + 4 + 1)

    waits = []

    lx = []
    for s in range(2):
        for d in range(1, nxh):
            copy = send(
                lp_ref.at[s], lf.at[s, z * nxh + xh, core], lx_s.at[s, d], lx_r.at[s, d],
                pcol=xh_peer(d),
            )
            copy.start()
            lx.append(copy)
    waits += lx

    def reduce_start(s):
        copies = []
        for d in far:
            copy = send(
                rs_src.at[s, row_peer(d)], rs_dst.at[s, d], rs_s.at[s, d], rs_r.at[s, d],
                prow=row_peer(d),
            )
            copy.start()
            copies.append(copy)
        waits.extend(copies)
        return copies

    def reduce_finish(s, copies):
        total = rs_src[s, me]
        for d, copy in reversed(list(zip(far, copies))):
            copy.wait_recv()
            total = total + rs_dst[s, d]
        mine = pl.ds(pl.multiple_of(me * chunk, chunk), chunk)
        x_buf[s, mine, :] = total

    def gather_start(s):
        mine = pl.ds(pl.multiple_of(me * chunk, chunk), chunk)
        copies = []
        for d in far:
            copy = send(
                x_buf.at[s, mine], x_buf.at[s, mine], ag_s.at[s, d], ag_r.at[s, d],
                prow=row_peer(d),
            )
            copy.start()
            copies.append(copy)
        waits.extend(copies)
        return copies

    def top_start(s):
        copies = []
        for d in sorted(range(1, ny), key=lambda d: -min(d, ny - d)):
            piece = t_buf.at[s, y, x]
            copy = send(
                piece, piece, ta_s.at[s, d], ta_r.at[s, d], prow=lax.rem(y + d, ny) * 2 + x
            )
            copy.start()
            copies.append(copy)
        waits.extend(copies)
        return copies

    def top_forward(s, copies):
        for copy in copies:
            copy.wait_recv()
        copy = send(
            t_buf.at[s, :, x], t_buf.at[s, :, x], tf_s.at[s], tf_r.at[s], prow=y * 2 + 1 - x
        )
        copy.start()
        waits.append(copy)
        return copy

    def scatter_copies(src, s):
        copies = []
        for m in range(1, rows_n):
            rows = pl.ds(m * chunk, chunk)
            copies.append(
                send(
                    src.at[rows], t_buf.at[s, m // 2, m % 2], sc_s.at[s, m], sc_r.at[s],
                    prow=jnp.int32(m),
                )
            )
        return copies

    def scatter_wait(s):
        piece = t_buf.at[s, y, x]

        @pl.when(jnp.logical_not(is_root))
        def _():
            send(piece, piece, sc_s.at[s, 0], sc_r.at[s], prow=row_peer(1)).wait_recv()

    rs0 = reduce_start(0)

    @pl.when(is_root)
    def _():
        own_t.start()
        for copy in scatter_copies(a_ref, 0):
            copy.start()

    z1[...] = pick(source(col1))

    @pl.when(is_root)
    def _():
        wanted = source(sub + nb)
        onehot = (wanted == lane).astype(F32)
        moved = select(onehot.astype(BF16), a_ref[pl.ds(0, nb), :])
        swapped = jnp.max(onehot, axis=1, keepdims=True) > 0
        d_top[...] = jnp.where(swapped, moved, a_ref[pl.ds(nb, nb), :])

    turn = 1 - 2 * lax.rem(z, 2)
    routes = (
        (0, 1), (0, -1), (0, 2), (0, -2), (-2, 1), (2, -1), (-2 * turn, 2 * turn)
    )

    def z_copy(s, q):
        held, there = routes[q]
        group = lf.at[s, pl.ds(z_at(held) * nxh, nxh), core]
        return send(group, group, lz_s.at[s, q], lz_r.at[s, q], pcol=z_peer(there))

    def panel_x(s):
        own[s].wait()
        for copy in lx[s * (nxh - 1): (s + 1) * (nxh - 1)]:
            copy.wait_recv()
        copies = [z_copy(s, q) for q in (2, 3, 0, 1)]
        for copy in copies:
            copy.start()
        waits.extend(copies)
        return copies

    def swap_start(s, offsets):
        copies = []
        for d in offsets:
            group = lf.at[s, pl.ds(z_at(d) * nxh, nxh), core]
            copies.append(
                send(group, group, lc_s.at[s, d + 3], lc_r.at[s, d + 3], pcol=partner)
            )
            copies[-1].start()
        waits.extend(copies)
        return copies

    def panel_pass(s, copies):
        for copy in copies:
            copy.wait_recv()
        copies = [z_copy(s, q) for q in (6, 4, 5)]
        for copy in copies:
            copy.start()
        waits.extend(copies)
        return copies, swap_start(s, (0, -1, 1, -2, 2))

    def panel_finish(s, copies, swaps):
        for copy in copies:
            copy.wait_recv()
        swaps = swaps + swap_start(s, (4, -3, 3))
        for copy in swaps:
            copy.wait_recv()

    def tops(s):
        return t_buf[s].reshape(nb, -1)

    lz0 = panel_x(0)

    reduce_finish(0, rs0)
    ag0 = gather_start(0)

    lz0 = panel_pass(0, lz0)

    scatter_wait(0)

    @pl.when(is_root)
    def _():
        own_t.wait()

    ta0 = top_start(0)

    def factor(s, b):
        per = nz * nxh // blocks
        return lf[s, pl.ds(b * per, per)].reshape(nb, nb)

    panel_finish(0, *lz0)
    lz1 = panel_x(1)
    l_sel = None
    for b in range(blocks):
        onehot = (col1 == lane + (first + b * nb)).astype(F32).astype(BF16)
        part = select(onehot, factor(0, b))
        l_sel = part if l_sel is None else l_sel + part

    for copy in ag0:
        copy.wait_recv()
    loads[2].wait()
    upper0 = matmul(linv_ref[0], x_buf[0])
    rs_src[1] = (z1[...] - matmul(l_sel, upper0)).reshape(rows_n, chunk, -1)
    rs1 = reduce_start(1)

    @pl.when(is_root)
    def _():
        d_top[...] = d_top[...] - matmul(factor(0, 1), upper0)
        t_buf[1, 0, 0] = d_top[pl.ds(0, chunk), :]
        for copy in scatter_copies(d_top, 1):
            copy.start()

    tf0 = top_forward(0, ta0)
    lz1 = panel_pass(1, lz1)
    tf0.wait_recv()

    for b in range(blocks):
        here = sub + (first + b * nb)
        hit = (here == row0).astype(F32)
        moved = select(hit.astype(BF16), tops(0))
        any_hit = jnp.max(hit, axis=1, keepdims=True) > 0
        kept = jnp.where(any_hit, moved, a_ref[pl.ds(b * nb, nb), :])
        base[pl.ds(b * nb, nb), :] = kept - matmul(factor(0, b), upper0)

    reduce_finish(1, rs1)
    ag1 = gather_start(1)
    scatter_wait(1)
    ta1 = top_start(1)

    panel_finish(1, *lz1)

    tf1 = top_forward(1, ta1)

    for copy in ag1:
        copy.wait_recv()
    upper1 = matmul(linv_ref[1], x_buf[1])
    upper1_high = upper1.astype(BF16)
    upper1_low = (upper1 - upper1_high.astype(F32)).astype(BF16)

    tf1.wait_recv()
    for b in range(blocks):
        here = sub + (first + b * nb)
        hit = (here == row1).astype(F32)
        moved = select(hit.astype(BF16), tops(1))
        any_hit = jnp.max(hit, axis=1, keepdims=True) > 0
        value = jnp.where(any_hit, moved, base[pl.ds(b * nb, nb), :])
        left = factor(1, b)
        high = left.astype(BF16)
        low = (left - high.astype(F32)).astype(BF16)
        change = jnp.dot(high, upper1_low, preferred_element_type=F32)
        change = change + jnp.dot(low, upper1_high, preferred_element_type=F32)
        change = change + jnp.dot(high, upper1_high, preferred_element_type=F32)
        value = value - change
        if b == 0:
            value = jnp.where(is_root, upper0, value)
        if b == 1:
            value = jnp.where(is_root, upper1, value)
        out_ref[pl.ds(b * nb, nb), :] = value

    for copy in waits:
        copy.wait_send()

    @pl.when(is_root)
    def _():
        for s, src in ((0, a_ref), (1, d_top)):
            for copy in scatter_copies(src, s):
                copy.wait_send()


def per_device(split, rows_n, matrix, l_panels, l_inverse, pivots):
    nz, nxh, nc = split
    rows_dev, cols_dev = matrix.shape
    nb = pivots.shape[1]
    chunk = nb // rows_n
    part = l_panels.shape[1]
    dma = pltpu.SemaphoreType.DMA
    vmem = pl.BlockSpec(memory_space=pltpu.VMEM)
    return pl.pallas_call(
        functools.partial(kernel, (rows_n, nz, nxh, nc, nb)),
        out_shape=jax.ShapeDtypeStruct(matrix.shape, F32),
        in_specs=[pl.BlockSpec(memory_space=pl.ANY)] * 4,
        out_specs=vmem,
        scratch_shapes=[
            pltpu.VMEM(matrix.shape, F32),
            pltpu.VMEM(l_inverse.shape, F32),
            pltpu.VMEM(pivots.shape, jnp.int32),
            pltpu.VMEM((2, rows_n, chunk, cols_dev), F32),
            pltpu.VMEM((2, rows_n, chunk, cols_dev), F32),
            pltpu.VMEM((2, nb, cols_dev), F32),
            pltpu.VMEM((2, rows_n // 2, 2, chunk, cols_dev), F32),
            pltpu.VMEM((nb, cols_dev), F32),
            pltpu.VMEM((2, nz * nxh, nc, part, nb), F32),
            pltpu.VMEM((nb, cols_dev), F32),
            pltpu.VMEM((rows_dev, cols_dev), F32),
            dma((2, rows_n)), dma((2, rows_n)),
            dma((2, rows_n)), dma((2, rows_n)),
            dma((2, rows_n)), dma((2,)),
            dma((2, rows_n)), dma((2, rows_n)),
            dma((2,)), dma((2,)),
            dma((2, nxh)), dma((2, nxh)),
            dma((2, nz)), dma((2, nz)),
            dma((2, nz)), dma((2, nz)),
            dma((3,)), dma((3,)),
        ],
        compiler_params=pltpu.CompilerParams(
            collective_id=0, has_side_effects=True, vmem_limit_bytes=48 * 1024 * 1024
        ),
    )(matrix, l_panels, l_inverse, pivots)


def solution(mesh):
    placed = (P("prow", "pcol"), P(None, ("prow", "pcol"), None), P(), P())
    body = functools.partial(per_device, split_cols(mesh), mesh.shape["prow"])
    return jax.shard_map(
        body, mesh=mesh, in_specs=placed, out_specs=P("prow", "pcol"), check_vma=False
    )
```

```python
import functools

import jax
import jax.numpy as jnp
from jax import lax
from jax.experimental import pallas as pl
from jax.experimental.pallas import tpu as pltpu
from jax.sharding import PartitionSpec as P

MESH = pl.DeviceIdType.MESH
HIGHEST = lax.Precision.HIGHEST
F32 = jnp.float32
BF16 = jnp.bfloat16
VMEM_LIMIT = 48 * 1024 * 1024


def split_cols(mesh):
    nz, core = 8, 2
    return nz, mesh.shape["pcol"] // (nz * core), core


def select(onehot, values):
    high = values.astype(BF16)
    rest = values - high.astype(F32)
    mid = rest.astype(BF16)
    low = (rest - mid.astype(F32)).astype(BF16)
    out = jnp.dot(onehot, high, preferred_element_type=F32)
    out = out + jnp.dot(onehot, mid, preferred_element_type=F32)
    return out + jnp.dot(onehot, low, preferred_element_type=F32)


def split(values):
    high = values.astype(BF16)
    return high, (values - high.astype(F32)).astype(BF16)


def product(a, b):
    out = jnp.dot(a[0], b[1], preferred_element_type=F32)
    out = out + jnp.dot(a[1], b[0], preferred_element_type=F32)
    return out + jnp.dot(a[0], b[0], preferred_element_type=F32)


def matmul(a, b):
    return jnp.dot(a, b, precision=HIGHEST, preferred_element_type=F32)


def kernel(
    sizes, a_hbm, lp_ref, linv_hbm, piv_hbm, out_ref,
    a_ref, linv_ref, piv_ref,
    rs_src, rs_dst, x_buf, t_buf, d_top, d_part, lt, lf, z1, base,
    rs_s, rs_r, ag_s, ag_r, sc_s, sc_r, ta_s, ta_r, tf_s, tf_r,
    lx_s, lx_r, lz_s, lz_r, lc_s, lc_r, lt_s, lt_r, own_sem, in_sem,
):
    rows_n, nz, nxh, nc, nb = sizes
    chunk = nb // rows_n
    ny = rows_n // 2
    blocks = a_ref.shape[0] // nb
    me = lax.axis_index("prow")
    col = lax.axis_index("pcol")
    y, x = me // 2, lax.rem(me, 2)
    core = lax.rem(col, nc)
    xh = lax.rem(col // nc, nxh)
    z = col // (nc * nxh)
    first = me * a_ref.shape[0]
    is_root = me == 0

    def row_peer(d):
        return lax.rem(me + d, rows_n)

    def xh_peer(d):
        return (z * nxh + lax.rem(xh + d, nxh)) * nc + core

    def z_at(d):
        return lax.rem(z + d + nz, nz)

    def z_peer(d):
        return (z_at(d) * nxh + xh) * nc + core

    far = sorted(range(1, rows_n), key=lambda d: -min(d, rows_n - d))

    partner = (z * nxh + xh) * nc + (1 - core)

    def send(src, dst, s, r, **where):
        copy = pltpu.make_async_remote_copy(
            src_ref=src, dst_ref=dst, send_sem=s, recv_sem=r,
            device_id=where, device_id_type=MESH,
        )
        return copy

    barrier = pltpu.get_barrier_semaphore()
    for d in range(1, rows_n):
        pl.semaphore_signal(barrier, inc=1, device_id={"prow": row_peer(d)}, device_id_type=MESH)
    for d in range(1, nxh):
        pl.semaphore_signal(barrier, inc=1, device_id={"pcol": xh_peer(d)}, device_id_type=MESH)
    for d in range(1, nz):
        pl.semaphore_signal(barrier, inc=1, device_id={"pcol": z_peer(d)}, device_id_type=MESH)
    pl.semaphore_signal(barrier, inc=1, device_id={"pcol": partner}, device_id_type=MESH)

    own = [
        pltpu.make_async_copy(lp_ref.at[s], lf.at[s, z * nxh + xh, core], own_sem.at[s])
        for s in range(2)
    ]
    own_t = pltpu.make_async_copy(a_ref.at[pl.ds(0, chunk)], t_buf.at[0, 0, 0], own_sem.at[2])
    loads = [
        pltpu.make_async_copy(src, dst, in_sem.at[n])
        for n, (src, dst) in enumerate(
            ((piv_hbm, piv_ref), (a_hbm, a_ref), (linv_hbm, linv_ref))
        )
    ]
    for copy in loads + own:
        copy.start()
    loads[0].wait()

    def as_row(s):
        return jnp.broadcast_to(piv_ref[pl.ds(s, 1), :], (nb, nb))

    row0, row1 = as_row(0), as_row(1)
    col0, col1 = row0.T, row1.T
    lane = lax.broadcasted_iota(jnp.int32, (nb, nb), 1)
    sub = lax.broadcasted_iota(jnp.int32, (nb, nb), 0)

    def source(wanted):
        hit = wanted == row0
        place = jnp.max(jnp.where(hit, lane, -1), axis=1, keepdims=True)
        place = jnp.broadcast_to(place, (nb, nb))
        return jnp.where(place >= 0, place, wanted)

    def pick(wanted):
        total = None
        for b in range(blocks):
            onehot = (wanted == lane + (first + b * nb)).astype(F32).astype(BF16)
            part = select(onehot, a_ref[pl.ds(b * nb, nb), :])
            total = part if total is None else total + part
        return total

    loads[1].wait()
    rs_src[0] = pick(col0).reshape(rows_n, chunk, -1)

    pl.semaphore_wait(barrier, (rows_n - 1) + (nxh - 1) + (nz - 1) + 1)

    waits = []

    def panel_start(s):
        copies = []
        for d in sorted(range(1, nxh), key=lambda d: -min(d, nxh - d)):
            copy = send(
                lp_ref.at[s], lf.at[s, z * nxh + xh, core], lx_s.at[s, d], lx_r.at[s, d],
                pcol=xh_peer(d),
            )
            copy.start()
            copies.append(copy)
        waits.extend(copies)
        return copies

    lx0 = panel_start(0)

    first_top = nb // chunk
    top_col = first_top + me
    in_line = (z == top_col // (nxh * nc)) & (core == lax.rem(top_col, nc))
    at_source = in_line & (xh == lax.rem(top_col // nc, nxh))
    target = col - first_top

    def lt_copy(n, stage, **where):
        return send(lt, lt, lt_s.at[n], lt_r.at[stage], **where)

    lt_x = [lt_copy(d, 1, pcol=xh_peer(d)) for d in range(1, nxh)]
    lt_z = [lt_copy(nxh + d - 1, 2, pcol=z_peer(d)) for d in range(1, nz)]
    lt_c = lt_copy(nxh + nz - 1, 3, pcol=partner)
    lt_out = is_root & (target > 0) & (target < rows_n)
    lt_first = send(lp_ref.at[0], lt, lt_s.at[0], lt_r.at[0], prow=lax.rem(target + rows_n, rows_n))
    lt_own = pltpu.make_async_copy(lp_ref.at[0], lt, in_sem.at[3])

    def top_panel_first():
        @pl.when(lt_out)
        def _():
            lt_first.start()

        @pl.when(is_root & at_source)
        def _():
            lt_own.start()

    def top_panel_x():
        @pl.when(is_root & at_source)
        def _():
            lt_own.wait()

        @pl.when(jnp.logical_not(is_root) & at_source)
        def _():
            lt_first.wait_recv()

        @pl.when(at_source)
        def _():
            for copy in lt_x:
                copy.start()

    def top_panel_z():
        @pl.when(in_line & jnp.logical_not(at_source))
        def _():
            lt_x[0].wait_recv()

        @pl.when(in_line)
        def _():
            for copy in lt_z:
                copy.start()

    same_core = core == lax.rem(top_col, nc)

    def top_panel_core():
        @pl.when(same_core & jnp.logical_not(in_line))
        def _():
            lt_z[0].wait_recv()

        @pl.when(same_core)
        def _():
            lt_c.start()

    def top_panel_finish():
        @pl.when(jnp.logical_not(same_core))
        def _():
            lt_c.wait_recv()

    def top_panel_sent():
        @pl.when(lt_out)
        def _():
            lt_first.wait_send()

        @pl.when(at_source)
        def _():
            for copy in lt_x:
                copy.wait_send()

        @pl.when(in_line)
        def _():
            for copy in lt_z:
                copy.wait_send()

        @pl.when(same_core)
        def _():
            lt_c.wait_send()

    def reduce_start(s):
        copies = []
        for d in far:
            copy = send(
                rs_src.at[s, row_peer(d)], rs_dst.at[s, d], rs_s.at[s, d], rs_r.at[s, d],
                prow=row_peer(d),
            )
            copy.start()
            copies.append(copy)
        waits.extend(copies)
        return copies

    def reduce_finish(s, copies):
        total = rs_src[s, me]
        for d, copy in reversed(list(zip(far, copies))):
            copy.wait_recv()
            total = total + rs_dst[s, d]
        mine = pl.ds(pl.multiple_of(me * chunk, chunk), chunk)
        x_buf[s, mine, :] = total

    def gather_start(s):
        mine = pl.ds(pl.multiple_of(me * chunk, chunk), chunk)
        copies = []
        for d in far:
            copy = send(
                x_buf.at[s, mine], x_buf.at[s, mine], ag_s.at[s, d], ag_r.at[s, d],
                prow=row_peer(d),
            )
            copy.start()
            copies.append(copy)
        waits.extend(copies)
        return copies

    def top_start(s):
        copies = []
        for d in sorted(range(1, ny), key=lambda d: -min(d, ny - d)):
            piece = t_buf.at[s, y, x]
            copy = send(
                piece, piece, ta_s.at[s, d], ta_r.at[s, d], prow=lax.rem(y + d, ny) * 2 + x
            )
            copy.start()
            copies.append(copy)
        waits.extend(copies)
        return copies

    def top_forward(s, copies):
        for copy in copies:
            copy.wait_recv()
        copy = send(
            t_buf.at[s, :, x], t_buf.at[s, :, x], tf_s.at[s], tf_r.at[s], prow=y * 2 + 1 - x
        )
        copy.start()
        waits.append(copy)
        return copy

    def scatter_copies():
        copies = []
        for m in range(1, rows_n):
            rows = pl.ds(m * chunk, chunk)
            for s, (src, dst) in enumerate(
                ((a_ref.at[rows], t_buf.at[0, m // 2, m % 2]), (d_top.at[rows], d_part))
            ):
                copies.append(send(src, dst, sc_s.at[s, m], sc_r.at[s], prow=jnp.int32(m)))
        return copies

    def scatter_wait(s):
        piece = (t_buf.at[0, y, x], d_part)[s]

        @pl.when(jnp.logical_not(is_root))
        def _():
            send(piece, piece, sc_s.at[s, 0], sc_r.at[s], prow=row_peer(1)).wait_recv()

    rs0 = reduce_start(0)
    top_panel_first()

    z1[...] = pick(source(col1))

    @pl.when(is_root)
    def _():
        wanted = source(sub + nb)
        onehot = (wanted == lane).astype(F32)
        moved = select(onehot.astype(BF16), a_ref[pl.ds(0, nb), :])
        swapped = jnp.max(onehot, axis=1, keepdims=True) > 0
        d_top[...] = jnp.where(swapped, moved, a_ref[pl.ds(nb, nb), :])
        d_part[...] = d_top[pl.ds(0, chunk), :]

    turn = 1 - 2 * lax.rem(z, 2)
    routes = (
        (0, 1), (0, -1), (0, 2), (0, -2), (-2, 1), (2, -1), (-2 * turn, 2 * turn)
    )

    def z_copy(s, q):
        held, there = routes[q]
        group = lf.at[s, pl.ds(z_at(held) * nxh, nxh), core]
        return send(group, group, lz_s.at[s, q], lz_r.at[s, q], pcol=z_peer(there))

    def panel_x(s, lx):
        own[s].wait()
        for copy in lx:
            copy.wait_recv()
        copies = [z_copy(s, q) for q in (2, 3, 0, 1)]
        for copy in copies:
            copy.start()
        waits.extend(copies)
        return copies

    def swap_start(s, offsets):
        copies = []
        for d in offsets:
            group = lf.at[s, pl.ds(z_at(d) * nxh, nxh), core]
            copies.append(
                send(group, group, lc_s.at[s, d + 3], lc_r.at[s, d + 3], pcol=partner)
            )
            copies[-1].start()
        waits.extend(copies)
        return copies

    def panel_pass(s, copies):
        copies[0].wait_recv()
        copies[1].wait_recv()
        passed = [z_copy(s, q) for q in (6, 4, 5)]
        for copy in passed:
            copy.start()
        waits.extend(passed)
        swaps = swap_start(s, (0, -2, 2))
        copies[2].wait_recv()
        copies[3].wait_recv()
        return passed, swaps + swap_start(s, (-1, 1))

    def panel_finish(s, copies, swaps):
        for copy, d in zip(copies[1:] + copies[:1], (-3, 3, 4)):
            copy.wait_recv()
            swaps = swaps + swap_start(s, (d,))
        for copy in swaps:
            copy.wait_recv()

    def tops(s):
        return t_buf[s].reshape(nb, -1)

    lz0 = panel_x(0, lx0)

    reduce_finish(0, rs0)
    ag0 = gather_start(0)

    @pl.when(is_root)
    def _():
        own_t.start()
        for copy in scatter_copies():
            copy.start()

    top_panel_x()
    lx1 = panel_start(1)

    lz0 = panel_pass(0, lz0)

    top_panel_z()
    scatter_wait(0)

    @pl.when(is_root)
    def _():
        own_t.wait()

    ta0 = top_start(0)

    def factor(s, b):
        per = nz * nxh // blocks
        return lf[s, pl.ds(b * per, per)].reshape(nb, nb)

    top_panel_core()
    panel_finish(0, *lz0)
    lz1 = panel_x(1, lx1)
    l_sel = None
    for b in range(blocks):
        onehot = (col1 == lane + (first + b * nb)).astype(F32).astype(BF16)
        part = select(onehot, factor(0, b))
        l_sel = part if l_sel is None else l_sel + part
    l_sel = split(l_sel)

    for copy in ag0:
        copy.wait_recv()
    loads[2].wait()
    upper0 = matmul(linv_ref[0], x_buf[0])
    upper0_parts = split(upper0)
    rs_src[1] = (z1[...] - product(l_sel, upper0_parts)).reshape(rows_n, chunk, -1)
    rs1 = reduce_start(1)

    top_panel_finish()
    scatter_wait(1)
    t_buf[1, y, x] = d_part[...] - product(split(lt[...]), upper0_parts)
    ta1 = top_start(1)

    tf0 = top_forward(0, ta0)

    for b in range(blocks):
        rows = pl.ds(b * nb, nb)
        base[rows, :] = product(split(factor(0, b)), upper0_parts)

    lz1 = panel_pass(1, lz1)

    tf0.wait_recv()
    for b in range(blocks):
        rows = pl.ds(b * nb, nb)
        hit = (sub + (first + b * nb) == row0).astype(F32)
        moved = select(hit.astype(BF16), tops(0))
        any_hit = jnp.max(hit, axis=1, keepdims=True) > 0
        base[rows, :] = jnp.where(any_hit, moved, a_ref[rows, :]) - base[rows, :]

    reduce_finish(1, rs1)
    ag1 = gather_start(1)

    panel_finish(1, *lz1)

    tf1 = top_forward(1, ta1)
    tf1.wait_recv()
    for b in range(blocks):
        rows = pl.ds(b * nb, nb)
        hit = (sub + (first + b * nb) == row1).astype(F32)
        moved = select(hit.astype(BF16), tops(1))
        any_hit = jnp.max(hit, axis=1, keepdims=True) > 0
        base[rows, :] = jnp.where(any_hit, moved, base[rows, :])

    for copy in ag1:
        copy.wait_recv()
    upper1 = matmul(linv_ref[1], x_buf[1])
    upper1_parts = split(upper1)
    for b in range(blocks):
        rows = pl.ds(b * nb, nb)
        value = base[rows, :] - product(split(factor(1, b)), upper1_parts)
        if b == 0:
            value = jnp.where(is_root, upper0, value)
        if b == 1:
            value = jnp.where(is_root, upper1, value)
        out_ref[rows, :] = value

    for copy in waits:
        copy.wait_send()

    top_panel_sent()

    @pl.when(is_root)
    def _():
        for copy in scatter_copies():
            copy.wait_send()


def per_device(split, rows_n, matrix, l_panels, l_inverse, pivots):
    nz, nxh, nc = split
    rows_dev, cols_dev = matrix.shape
    nb = pivots.shape[1]
    chunk = nb // rows_n
    part = l_panels.shape[1]
    dma = pltpu.SemaphoreType.DMA
    vmem = pl.BlockSpec(memory_space=pltpu.VMEM)
    return pl.pallas_call(
        functools.partial(kernel, (rows_n, nz, nxh, nc, nb)),
        out_shape=jax.ShapeDtypeStruct(matrix.shape, F32),
        in_specs=[pl.BlockSpec(memory_space=pltpu.HBM)] * 4,
        out_specs=vmem,
        scratch_shapes=[
            pltpu.VMEM(matrix.shape, F32),
            pltpu.VMEM(l_inverse.shape, F32),
            pltpu.VMEM(pivots.shape, jnp.int32),
            pltpu.VMEM((2, rows_n, chunk, cols_dev), F32),
            pltpu.VMEM((2, rows_n, chunk, cols_dev), F32),
            pltpu.VMEM((2, nb, cols_dev), F32),
            pltpu.VMEM((2, rows_n // 2, 2, chunk, cols_dev), F32),
            pltpu.VMEM((nb, cols_dev), F32),
            pltpu.VMEM((chunk, cols_dev), F32),
            pltpu.VMEM((part, nb), F32),
            pltpu.VMEM((2, nz * nxh, nc, part, nb), F32),
            pltpu.VMEM((nb, cols_dev), F32),
            pltpu.VMEM((rows_dev, cols_dev), F32),
            dma((2, rows_n)), dma((2, rows_n)),
            dma((2, rows_n)), dma((2, rows_n)),
            dma((2, rows_n)), dma((2,)),
            dma((2, rows_n)), dma((2, rows_n)),
            dma((2,)), dma((2,)),
            dma((2, nxh)), dma((2, nxh)),
            dma((2, nz)), dma((2, nz)),
            dma((2, nz)), dma((2, nz)),
            dma((nxh + nz,)), dma((4,)),
            dma((3,)), dma((4,)),
        ],
        compiler_params=pltpu.CompilerParams(
            collective_id=0, has_side_effects=True, vmem_limit_bytes=VMEM_LIMIT
        ),
    )(*[
        pltpu.with_memory_space_constraint(v, pltpu.HBM)
        for v in (matrix, l_panels, l_inverse, pivots)
    ])


def solution(mesh):
    placed = (P("prow", "pcol"), P(None, ("prow", "pcol"), None), P(), P())
    body = functools.partial(per_device, split_cols(mesh), mesh.shape["prow"])
    return jax.shard_map(
        body, mesh=mesh, in_specs=placed, out_specs=P("prow", "pcol"), check_vma=False
    )
```

```python
import functools

import jax
import jax.numpy as jnp
from jax import lax
from jax.experimental import pallas as pl
from jax.experimental.pallas import tpu as pltpu
from jax.sharding import PartitionSpec as P

MESH = pl.DeviceIdType.MESH
HIGHEST = lax.Precision.HIGHEST
F32 = jnp.float32
BF16 = jnp.bfloat16
VMEM_LIMIT = 48 * 1024 * 1024


def split_cols(mesh):
    nz, core = 8, 2
    return nz, mesh.shape["pcol"] // (nz * core), core


def select(onehot, values):
    high = values.astype(BF16)
    rest = values - high.astype(F32)
    mid = rest.astype(BF16)
    low = (rest - mid.astype(F32)).astype(BF16)
    out = jnp.dot(onehot, high, preferred_element_type=F32)
    out = out + jnp.dot(onehot, mid, preferred_element_type=F32)
    return out + jnp.dot(onehot, low, preferred_element_type=F32)


def split(values):
    high = values.astype(BF16)
    return high, (values - high.astype(F32)).astype(BF16)


def product(a, b):
    out = jnp.dot(a[0], b[1], preferred_element_type=F32)
    out = out + jnp.dot(a[1], b[0], preferred_element_type=F32)
    return out + jnp.dot(a[0], b[0], preferred_element_type=F32)


def matmul(a, b):
    return jnp.dot(a, b, precision=HIGHEST, preferred_element_type=F32)


def kernel(
    sizes, a_hbm, lp_ref, linv_hbm, piv_hbm, out_ref,
    a_ref, linv_ref, piv_ref,
    rs_src, rs_dst, x_buf, t_buf, d_top, d_part, lt, lf, z1, base,
    rs_s, rs_r, ag_s, ag_r, sc_s, sc_r, ta_s, ta_r, tf_s, tf_r,
    lx_s, lx_r, lz_s, lz_r, lc_s, lc_r, lt_s, lt_r, own_sem, in_sem,
):
    rows_n, nz, nxh, nc, nb = sizes
    chunk = nb // rows_n
    ny = rows_n // 2
    blocks = a_ref.shape[0] // nb
    me = lax.axis_index("prow")
    col = lax.axis_index("pcol")
    y, x = me // 2, lax.rem(me, 2)
    core = lax.rem(col, nc)
    xh = lax.rem(col // nc, nxh)
    z = col // (nc * nxh)
    first = me * a_ref.shape[0]
    is_root = me == 0

    def row_peer(d):
        return lax.rem(me + d, rows_n)

    def xh_peer(d):
        return (z * nxh + lax.rem(xh + d, nxh)) * nc + core

    def z_at(d):
        return lax.rem(z + d + nz, nz)

    def z_peer(d):
        return (z_at(d) * nxh + xh) * nc + core

    far = sorted(range(1, rows_n), key=lambda d: -min(d, rows_n - d))

    partner = (z * nxh + xh) * nc + (1 - core)

    def send(src, dst, s, r, **where):
        copy = pltpu.make_async_remote_copy(
            src_ref=src, dst_ref=dst, send_sem=s, recv_sem=r,
            device_id=where, device_id_type=MESH,
        )
        return copy

    def arrived(ref, sem):
        send(ref, ref, sem, sem, pcol=partner).wait_recv()

    def sent(ref, sem):
        send(ref, ref, sem, sem, pcol=partner).wait_send()

    barrier = pltpu.get_barrier_semaphore()
    for d in range(1, rows_n):
        pl.semaphore_signal(barrier, inc=1, device_id={"prow": row_peer(d)}, device_id_type=MESH)
    for d in range(1, nxh):
        pl.semaphore_signal(barrier, inc=1, device_id={"pcol": xh_peer(d)}, device_id_type=MESH)
    for d in range(1, nz):
        pl.semaphore_signal(barrier, inc=1, device_id={"pcol": z_peer(d)}, device_id_type=MESH)
    pl.semaphore_signal(barrier, inc=1, device_id={"pcol": partner}, device_id_type=MESH)

    own = [
        pltpu.make_async_copy(lp_ref.at[s], lf.at[s, z * nxh + xh, core], own_sem.at[s])
        for s in range(2)
    ]
    own_t = pltpu.make_async_copy(a_ref.at[pl.ds(0, chunk)], t_buf.at[0, 0, 0], own_sem.at[2])
    loads = [
        pltpu.make_async_copy(src, dst, in_sem.at[n])
        for n, (src, dst) in enumerate(
            ((piv_hbm, piv_ref), (a_hbm, a_ref), (linv_hbm, linv_ref))
        )
    ]
    for copy in loads + own:
        copy.start()
    loads[0].wait()

    def as_row(s):
        return jnp.broadcast_to(piv_ref[pl.ds(s, 1), :], (nb, nb))

    row0, row1 = as_row(0), as_row(1)
    col0, col1 = row0.T, row1.T
    lane = lax.broadcasted_iota(jnp.int32, (nb, nb), 1)
    sub = lax.broadcasted_iota(jnp.int32, (nb, nb), 0)

    def source(wanted):
        hit = wanted == row0
        place = jnp.max(jnp.where(hit, lane, -1), axis=1, keepdims=True)
        place = jnp.broadcast_to(place, (nb, nb))
        return jnp.where(place >= 0, place, wanted)

    def pick(wanted):
        total = None
        for b in range(blocks):
            onehot = (wanted == lane + (first + b * nb)).astype(F32).astype(BF16)
            part = select(onehot, a_ref[pl.ds(b * nb, nb), :])
            total = part if total is None else total + part
        return total

    loads[1].wait()
    rs_src[0] = pick(col0).reshape(rows_n, chunk, -1)

    pl.semaphore_wait(barrier, (rows_n - 1) + (nxh - 1) + (nz - 1) + 1)

    def panel_start(s):
        copies = {}
        for d in sorted(range(1, nxh), key=lambda d: -min(d, nxh - d)):
            copies[d] = send(
                lp_ref.at[s], lf.at[s, z * nxh + xh, core], lx_s.at[s], lx_r.at[s, d],
                pcol=xh_peer(d),
            )
            copies[d].start()
        return copies

    turn = 1 - 2 * lax.rem(z, 2)
    routes = (
        (0, 1), (0, -1), (0, 2), (0, -2), (-2, 1), (2, -1), (-2 * turn, 2 * turn)
    )

    slots = sorted(range(nxh), key=lambda d: min(d, nxh - d))

    def z_start(s, d, kinds):
        copies = {}
        for q in kinds:
            held, there = routes[q]
            piece = lf.at[s, z_at(held) * nxh + lax.rem(xh + d, nxh), core]
            n = {0: nxh, 1: nxh, 2: d, 3: d}.get(q, nxh + q - 3)
            send(piece, piece, lz_s.at[s], lz_r.at[s, n], pcol=z_peer(there)).start()

    def panel_own(s):
        own[s].wait()
        z_start(s, 0, (2, 3))

    def panel_x(s, lx):
        for d in slots[1:]:
            lx[nxh - d].wait_recv()
            z_start(s, d, (2, 3))
        for d in slots:
            z_start(s, d, (0, 1))

    def swap_start(s, offsets):
        for d in offsets:
            group = lf.at[s, pl.ds(z_at(d) * nxh, nxh), core]
            send(group, group, lc_s.at[s], lc_r.at[s], pcol=partner).start()

    def panel_pass(s):
        for d in slots:
            arrived(lf.at[s, pl.ds(0, 2), 0], lz_r.at[s, d])
            z_start(s, d, (6, 4, 5))
        swap_start(s, (0, -2, 2))
        arrived(lf.at[s, pl.ds(0, 2 * nxh), 0], lz_r.at[s, nxh])
        swap_start(s, (-1, 1))

    def panel_finish(s):
        for q, d in ((4, -3), (5, 3), (6, 4)):
            arrived(lf.at[s, pl.ds(0, nxh), 0], lz_r.at[s, nxh + q - 3])
            swap_start(s, (d,))
        arrived(lf.at[s, :, 0], lc_r.at[s])

    lx0 = panel_start(0)
    panel_own(0)

    first_top = nb // chunk
    top_col = first_top + me
    in_line = (z == top_col // (nxh * nc)) & (core == lax.rem(top_col, nc))
    at_source = in_line & (xh == lax.rem(top_col // nc, nxh))
    target = col - first_top

    def lt_copy(stage, **where):
        return send(lt, lt, lt_s.at[stage], lt_r.at[stage], **where)

    lt_x = [lt_copy(1, pcol=xh_peer(d)) for d in range(1, nxh)]
    lt_z = [lt_copy(2, pcol=z_peer(d)) for d in range(1, nz)]
    lt_c = lt_copy(3, pcol=partner)
    lt_out = is_root & (target > 0) & (target < rows_n)
    lt_first = send(lp_ref.at[0], lt, lt_s.at[0], lt_r.at[0], prow=lax.rem(target + rows_n, rows_n))
    lt_own = pltpu.make_async_copy(lp_ref.at[0], lt, in_sem.at[3])

    def top_panel_first():
        @pl.when(lt_out)
        def _():
            lt_first.start()

        @pl.when(is_root & at_source)
        def _():
            lt_own.start()

    def top_panel_x():
        @pl.when(is_root & at_source)
        def _():
            lt_own.wait()

        @pl.when(jnp.logical_not(is_root) & at_source)
        def _():
            lt_first.wait_recv()

        @pl.when(at_source)
        def _():
            for copy in lt_x:
                copy.start()

    def top_panel_z():
        @pl.when(in_line & jnp.logical_not(at_source))
        def _():
            lt_x[0].wait_recv()

        @pl.when(in_line)
        def _():
            for copy in lt_z:
                copy.start()

    same_core = core == lax.rem(top_col, nc)

    def top_panel_core():
        @pl.when(same_core & jnp.logical_not(in_line))
        def _():
            lt_z[0].wait_recv()

        @pl.when(same_core)
        def _():
            lt_c.start()

    def top_panel_finish():
        @pl.when(jnp.logical_not(same_core))
        def _():
            lt_c.wait_recv()

    def top_panel_sent():
        @pl.when(lt_out)
        def _():
            lt_first.wait_send()

        @pl.when(at_source)
        def _():
            sent(lf.at[0, pl.ds(0, nxh - 1), 0], lt_s.at[1])

        @pl.when(in_line)
        def _():
            sent(lf.at[0, pl.ds(0, nz - 1), 0], lt_s.at[2])

        @pl.when(same_core)
        def _():
            lt_c.wait_send()

    def reduce_start(s):
        for d in far:
            send(
                rs_src.at[s, row_peer(d)], rs_dst.at[s, d], rs_s.at[s], rs_r.at[s],
                prow=row_peer(d),
            ).start()

    def reduce_finish(s):
        arrived(rs_dst.at[s, pl.ds(1, rows_n - 1)], rs_r.at[s])
        total = rs_src[s, me]
        for d in range(1, rows_n):
            total = total + rs_dst[s, d]
        mine = pl.ds(pl.multiple_of(me * chunk, chunk), chunk)
        x_buf[s, mine, :] = total

    others = pl.ds(0, (rows_n - 1) * chunk)

    def gather_start(s):
        mine = pl.ds(pl.multiple_of(me * chunk, chunk), chunk)
        for d in far:
            send(
                x_buf.at[s, mine], x_buf.at[s, mine], ag_s.at[s], ag_r.at[s], prow=row_peer(d)
            ).start()

    def top_start(s):
        for d in sorted(range(1, ny), key=lambda d: -min(d, ny - d)):
            piece = t_buf.at[s, y, x]
            send(
                piece, piece, ta_s.at[s], ta_r.at[s], prow=lax.rem(y + d, ny) * 2 + x
            ).start()

    def top_forward(s):
        arrived(t_buf.at[s, pl.ds(0, ny - 1), 0], ta_r.at[s])
        copy = send(
            t_buf.at[s, :, x], t_buf.at[s, :, x], tf_s.at[s], tf_r.at[s], prow=y * 2 + 1 - x
        )
        copy.start()
        return copy

    def scatter_copies(s):
        copies = []
        for m in sorted(range(1, rows_n), key=lambda m: -min(m, rows_n - m)):
            rows = pl.ds(m * chunk, chunk)
            src = (a_ref, d_top)[s].at[rows]
            dst = (t_buf.at[0, m // 2, m % 2], d_part)[s]
            copies.append(send(src, dst, sc_s.at[s], sc_r.at[s], prow=jnp.int32(m)))
        return copies

    def scatter_wait(s):
        piece = (t_buf.at[0, y, x], d_part)[s]

        @pl.when(jnp.logical_not(is_root))
        def _():
            arrived(piece, sc_r.at[s])

    reduce_start(0)
    top_panel_first()

    z1[...] = pick(source(col1))

    @pl.when(is_root)
    def _():
        wanted = source(sub + nb)
        onehot = (wanted == lane).astype(F32)
        moved = select(onehot.astype(BF16), a_ref[pl.ds(0, nb), :])
        swapped = jnp.max(onehot, axis=1, keepdims=True) > 0
        d_top[...] = jnp.where(swapped, moved, a_ref[pl.ds(nb, nb), :])
        d_part[...] = d_top[pl.ds(0, chunk), :]

    def tops(s):
        return t_buf[s].reshape(nb, -1)

    panel_x(0, lx0)

    reduce_finish(0)
    gather_start(0)

    @pl.when(is_root)
    def _():
        own_t.start()
        for copy in scatter_copies(0):
            copy.start()

    top_panel_x()
    lx1 = panel_start(1)

    panel_pass(0)

    @pl.when(is_root)
    def _():
        for copy in scatter_copies(1):
            copy.start()

    top_panel_z()
    scatter_wait(0)

    @pl.when(is_root)
    def _():
        own_t.wait()

    top_start(0)

    def factor(s, b):
        per = nz * nxh // blocks
        return lf[s, pl.ds(b * per, per)].reshape(nb, nb)

    top_panel_core()
    panel_finish(0)
    panel_own(1)
    panel_x(1, lx1)
    l_sel = None
    for b in range(blocks):
        onehot = (col1 == lane + (first + b * nb)).astype(F32).astype(BF16)
        part = select(onehot, factor(0, b))
        l_sel = part if l_sel is None else l_sel + part
    l_sel = split(l_sel)

    arrived(x_buf.at[0, others], ag_r.at[0])
    loads[2].wait()
    upper0 = matmul(linv_ref[0], x_buf[0])
    upper0_parts = split(upper0)
    rs_src[1] = (z1[...] - product(l_sel, upper0_parts)).reshape(rows_n, chunk, -1)
    reduce_start(1)

    top_panel_finish()
    scatter_wait(1)
    t_buf[1, y, x] = d_part[...] - product(split(lt[...]), upper0_parts)
    top_start(1)

    tf0 = top_forward(0)

    for b in range(blocks):
        rows = pl.ds(b * nb, nb)
        base[rows, :] = product(split(factor(0, b)), upper0_parts)

    panel_pass(1)

    reduce_finish(1)
    gather_start(1)
    tf1 = top_forward(1)

    panel_finish(1)

    tf0.wait_recv()
    for b in range(blocks):
        rows = pl.ds(b * nb, nb)
        hit = (sub + (first + b * nb) == row0).astype(F32)
        moved = select(hit.astype(BF16), tops(0))
        any_hit = jnp.max(hit, axis=1, keepdims=True) > 0
        base[rows, :] = jnp.where(any_hit, moved, a_ref[rows, :]) - base[rows, :]

    tf1.wait_recv()
    for b in range(blocks):
        rows = pl.ds(b * nb, nb)
        hit = (sub + (first + b * nb) == row1).astype(F32)
        moved = select(hit.astype(BF16), tops(1))
        any_hit = jnp.max(hit, axis=1, keepdims=True) > 0
        base[rows, :] = jnp.where(any_hit, moved, base[rows, :])

    arrived(x_buf.at[1, others], ag_r.at[1])
    upper1 = matmul(linv_ref[1], x_buf[1])
    upper1_parts = split(upper1)
    for b in range(blocks):
        rows = pl.ds(b * nb, nb)
        value = base[rows, :] - product(split(factor(1, b)), upper1_parts)
        if b == 0:
            value = jnp.where(is_root, upper0, value)
        if b == 1:
            value = jnp.where(is_root, upper1, value)
        out_ref[rows, :] = value

    for s in range(2):
        sent(lf.at[s, pl.ds(0, nxh - 1), 0], lx_s.at[s])
        sent(lf.at[s, pl.ds(0, (nz - 1) * nxh), 0], lz_s.at[s])
        sent(lf.at[s, :, 0], lc_s.at[s])
        sent(rs_src.at[s, pl.ds(1, rows_n - 1)], rs_s.at[s])
        sent(x_buf.at[s, others], ag_s.at[s])
        sent(t_buf.at[s, pl.ds(0, ny - 1), 0], ta_s.at[s])
    tf0.wait_send()
    tf1.wait_send()

    top_panel_sent()

    @pl.when(is_root)
    def _():
        for s in range(2):
            sent(d_top.at[others], sc_s.at[s])


def per_device(split, rows_n, matrix, l_panels, l_inverse, pivots):
    nz, nxh, nc = split
    rows_dev, cols_dev = matrix.shape
    nb = pivots.shape[1]
    chunk = nb // rows_n
    part = l_panels.shape[1]
    dma = pltpu.SemaphoreType.DMA
    vmem = pl.BlockSpec(memory_space=pltpu.VMEM)
    return pl.pallas_call(
        functools.partial(kernel, (rows_n, nz, nxh, nc, nb)),
        out_shape=jax.ShapeDtypeStruct(matrix.shape, F32),
        in_specs=[pl.BlockSpec(memory_space=pltpu.HBM)] * 4,
        out_specs=vmem,
        scratch_shapes=[
            pltpu.VMEM(matrix.shape, F32),
            pltpu.VMEM(l_inverse.shape, F32),
            pltpu.VMEM(pivots.shape, jnp.int32),
            pltpu.VMEM((2, rows_n, chunk, cols_dev), F32),
            pltpu.VMEM((2, rows_n, chunk, cols_dev), F32),
            pltpu.VMEM((2, nb, cols_dev), F32),
            pltpu.VMEM((2, rows_n // 2, 2, chunk, cols_dev), F32),
            pltpu.VMEM((nb, cols_dev), F32),
            pltpu.VMEM((chunk, cols_dev), F32),
            pltpu.VMEM((part, nb), F32),
            pltpu.VMEM((2, nz * nxh, nc, part, nb), F32),
            pltpu.VMEM((nb, cols_dev), F32),
            pltpu.VMEM((rows_dev, cols_dev), F32),
            dma((2,)), dma((2,)), dma((2,)), dma((2,)),
            dma((2,)), dma((2,)), dma((2,)), dma((2,)), dma((2,)), dma((2,)),
            dma((2,)), dma((2, nxh)), dma((2,)), dma((2, nxh + 4)), dma((2,)), dma((2,)),
            dma((4,)), dma((4,)),
            dma((3,)), dma((4,)),
        ],
        compiler_params=pltpu.CompilerParams(
            collective_id=0, has_side_effects=True, vmem_limit_bytes=VMEM_LIMIT
        ),
    )(*[
        pltpu.with_memory_space_constraint(v, pltpu.HBM)
        for v in (matrix, l_panels, l_inverse, pivots)
    ])


def solution(mesh):
    placed = (P("prow", "pcol"), P(None, ("prow", "pcol"), None), P(), P())
    body = functools.partial(per_device, split_cols(mesh), mesh.shape["prow"])
    return jax.shard_map(
        body, mesh=mesh, in_specs=placed, out_specs=P("prow", "pcol"), check_vma=False
    )
```

```python
import functools

import jax
import jax.numpy as jnp
from jax import lax
from jax.experimental import pallas as pl
from jax.experimental.pallas import tpu as pltpu
from jax.sharding import PartitionSpec as P

MESH = pl.DeviceIdType.MESH
HIGHEST = lax.Precision.HIGHEST
F32 = jnp.float32
BF16 = jnp.bfloat16
VMEM_LIMIT = 48 * 1024 * 1024


def split_cols(mesh):
    nz, core = 8, 2
    return nz, mesh.shape["pcol"] // (nz * core), core


def select(onehot, values):
    high = values.astype(BF16)
    rest = values - high.astype(F32)
    mid = rest.astype(BF16)
    low = (rest - mid.astype(F32)).astype(BF16)
    out = jnp.dot(onehot, high, preferred_element_type=F32)
    out = out + jnp.dot(onehot, mid, preferred_element_type=F32)
    return out + jnp.dot(onehot, low, preferred_element_type=F32)


def split(values):
    high = values.astype(BF16)
    return high, (values - high.astype(F32)).astype(BF16)


def product(a, b):
    out = jnp.dot(a[0], b[1], preferred_element_type=F32)
    out = out + jnp.dot(a[1], b[0], preferred_element_type=F32)
    return out + jnp.dot(a[0], b[0], preferred_element_type=F32)


def matmul(a, b):
    return jnp.dot(a, b, precision=HIGHEST, preferred_element_type=F32)


def kernel(
    sizes, a_hbm, lp_ref, linv_hbm, piv_hbm, out_ref,
    a_ref, linv_ref, piv_ref,
    rs_src, rs_dst, x_buf, t_buf, d_top, d_part, lt, lf, z1, base,
    rs_s, rs_r, ag_s, ag_r, sc_s, sc_r, ta_s, ta_r, tf_s, tf_r,
    lx_s, lx_r, lz_s, lz_r, lc_s, lc_r, lt_s, lt_r, own_sem, in_sem,
):
    rows_n, nz, nxh, nc, nb = sizes
    chunk = nb // rows_n
    ny = rows_n // 2
    blocks = a_ref.shape[0] // nb
    me = lax.axis_index("prow")
    col = lax.axis_index("pcol")
    y, x = me // 2, lax.rem(me, 2)
    core = lax.rem(col, nc)
    xh = lax.rem(col // nc, nxh)
    z = col // (nc * nxh)
    first = me * a_ref.shape[0]
    is_root = me == 0

    def row_peer(d):
        return lax.rem(me + d, rows_n)

    def xh_peer(d):
        return (z * nxh + lax.rem(xh + d, nxh)) * nc + core

    def z_at(d):
        return lax.rem(z + d + nz, nz)

    def z_peer(d):
        return (z_at(d) * nxh + xh) * nc + core

    far = sorted(range(1, rows_n), key=lambda d: -min(d, rows_n - d))

    partner = (z * nxh + xh) * nc + (1 - core)

    def send(src, dst, s, r, **where):
        copy = pltpu.make_async_remote_copy(
            src_ref=src, dst_ref=dst, send_sem=s, recv_sem=r,
            device_id=where, device_id_type=MESH,
        )
        return copy

    def arrived(ref, sem):
        send(ref, ref, sem, sem, pcol=partner).wait_recv()

    def sent(ref, sem):
        send(ref, ref, sem, sem, pcol=partner).wait_send()

    barrier = pltpu.get_barrier_semaphore()
    for d in range(1, rows_n):
        pl.semaphore_signal(barrier, inc=1, device_id={"prow": row_peer(d)}, device_id_type=MESH)
    for d in range(1, nxh):
        pl.semaphore_signal(barrier, inc=1, device_id={"pcol": xh_peer(d)}, device_id_type=MESH)
    for d in range(1, nz):
        pl.semaphore_signal(barrier, inc=1, device_id={"pcol": z_peer(d)}, device_id_type=MESH)
    pl.semaphore_signal(barrier, inc=1, device_id={"pcol": partner}, device_id_type=MESH)

    own = [
        pltpu.make_async_copy(lp_ref.at[s], lf.at[s, z * nxh + xh, core], own_sem.at[s])
        for s in range(2)
    ]
    own_t = pltpu.make_async_copy(a_ref.at[pl.ds(0, chunk)], t_buf.at[0, 0, 0], own_sem.at[2])
    loads = [
        pltpu.make_async_copy(src, dst, in_sem.at[n])
        for n, (src, dst) in enumerate(
            ((piv_hbm, piv_ref), (a_hbm, a_ref), (linv_hbm, linv_ref))
        )
    ]
    for copy in loads + own:
        copy.start()
    loads[0].wait()

    def as_row(s):
        return jnp.broadcast_to(piv_ref[pl.ds(s, 1), :], (nb, nb))

    row0, row1 = as_row(0), as_row(1)
    col0, col1 = row0.T, row1.T
    lane = lax.broadcasted_iota(jnp.int32, (nb, nb), 1)
    sub = lax.broadcasted_iota(jnp.int32, (nb, nb), 0)

    def source(wanted):
        hit = wanted == row0
        place = jnp.max(jnp.where(hit, lane, -1), axis=1, keepdims=True)
        place = jnp.broadcast_to(place, (nb, nb))
        return jnp.where(place >= 0, place, wanted)

    def pick(wanted):
        total = None
        for b in range(blocks):
            onehot = (wanted == lane + (first + b * nb)).astype(F32).astype(BF16)
            part = select(onehot, a_ref[pl.ds(b * nb, nb), :])
            total = part if total is None else total + part
        return total

    loads[1].wait()
    rs_src[0] = pick(col0).reshape(rows_n, chunk, -1)

    pl.semaphore_wait(barrier, (rows_n - 1) + (nxh - 1) + (nz - 1) + 1)

    def panel_start(s):
        copies = {}
        for d in sorted(range(1, nxh), key=lambda d: -min(d, nxh - d)):
            copies[d] = send(
                lp_ref.at[s], lf.at[s, z * nxh + xh, core], lx_s.at[s], lx_r.at[s, d],
                pcol=xh_peer(d),
            )
            copies[d].start()
        return copies

    turn = 1 - 2 * lax.rem(z, 2)
    routes = (
        (0, 1), (0, -1), (0, 2), (0, -2), (-2, 1), (2, -1), (-2 * turn, 2 * turn)
    )

    slots = sorted(range(nxh), key=lambda d: min(d, nxh - d))

    def z_start(s, d, kinds):
        copies = {}
        for q in kinds:
            held, there = routes[q]
            piece = lf.at[s, z_at(held) * nxh + lax.rem(xh + d, nxh), core]
            n = {0: nxh, 1: nxh, 2: d, 3: d}.get(q, nxh + q - 3)
            send(piece, piece, lz_s.at[s], lz_r.at[s, n], pcol=z_peer(there)).start()

    def panel_own(s):
        own[s].wait()
        z_start(s, 0, (2, 3))

    def panel_x(s, lx):
        for d in slots[1:]:
            lx[nxh - d].wait_recv()
            z_start(s, d, (2, 3))
        for d in slots:
            z_start(s, d, (0, 1))

    def swap_start(s, offsets):
        for d in offsets:
            group = lf.at[s, pl.ds(z_at(d) * nxh, nxh), core]
            send(group, group, lc_s.at[s], lc_r.at[s], pcol=partner).start()

    def panel_pass(s):
        for d in slots:
            arrived(lf.at[s, pl.ds(0, 2), 0], lz_r.at[s, d])
            z_start(s, d, (6, 4, 5))
        swap_start(s, (0, -2, 2))
        arrived(lf.at[s, pl.ds(0, 2 * nxh), 0], lz_r.at[s, nxh])
        swap_start(s, (-1, 1))

    def panel_finish(s):
        for q, d in ((4, -3), (5, 3), (6, 4)):
            arrived(lf.at[s, pl.ds(0, nxh), 0], lz_r.at[s, nxh + q - 3])
            swap_start(s, (d,))
        arrived(lf.at[s, :, 0], lc_r.at[s])

    lx0 = panel_start(0)
    panel_own(0)

    first_top = nb // chunk
    top_col = first_top + me
    in_line = (z == top_col // (nxh * nc)) & (core == lax.rem(top_col, nc))
    at_source = in_line & (xh == lax.rem(top_col // nc, nxh))
    target = col - first_top

    def lt_copy(stage, **where):
        return send(lt, lt, lt_s.at[stage], lt_r.at[stage], **where)

    lt_x = [lt_copy(1, pcol=xh_peer(d)) for d in range(1, nxh)]
    lt_z = [lt_copy(2, pcol=z_peer(d)) for d in range(1, nz)]
    lt_c = lt_copy(3, pcol=partner)
    lt_out = is_root & (target > 0) & (target < rows_n)
    lt_first = send(lp_ref.at[0], lt, lt_s.at[0], lt_r.at[0], prow=lax.rem(target + rows_n, rows_n))
    lt_own = pltpu.make_async_copy(lp_ref.at[0], lt, in_sem.at[3])

    def top_panel_first():
        @pl.when(lt_out)
        def _():
            lt_first.start()

        @pl.when(is_root & at_source)
        def _():
            lt_own.start()

    def top_panel_x():
        @pl.when(is_root & at_source)
        def _():
            lt_own.wait()

        @pl.when(jnp.logical_not(is_root) & at_source)
        def _():
            lt_first.wait_recv()

        @pl.when(at_source)
        def _():
            for copy in lt_x:
                copy.start()

    def top_panel_z():
        @pl.when(in_line & jnp.logical_not(at_source))
        def _():
            lt_x[0].wait_recv()

        @pl.when(in_line)
        def _():
            for copy in lt_z:
                copy.start()

    same_core = core == lax.rem(top_col, nc)

    def top_panel_core():
        @pl.when(same_core & jnp.logical_not(in_line))
        def _():
            lt_z[0].wait_recv()

        @pl.when(same_core)
        def _():
            lt_c.start()

    def top_panel_finish():
        @pl.when(jnp.logical_not(same_core))
        def _():
            lt_c.wait_recv()

    def top_panel_sent():
        @pl.when(lt_out)
        def _():
            lt_first.wait_send()

        @pl.when(at_source)
        def _():
            sent(lf.at[0, pl.ds(0, nxh - 1), 0], lt_s.at[1])

        @pl.when(in_line)
        def _():
            sent(lf.at[0, pl.ds(0, nz - 1), 0], lt_s.at[2])

        @pl.when(same_core)
        def _():
            lt_c.wait_send()

    def reduce_start(s):
        for d in far:
            send(
                rs_src.at[s, row_peer(d)], rs_dst.at[s, d], rs_s.at[s], rs_r.at[s],
                prow=row_peer(d),
            ).start()

    def reduce_finish(s):
        arrived(rs_dst.at[s, pl.ds(1, rows_n - 1)], rs_r.at[s])
        total = rs_src[s, me]
        for d in range(1, rows_n):
            total = total + rs_dst[s, d]
        mine = pl.ds(pl.multiple_of(me * chunk, chunk), chunk)
        x_buf[s, mine, :] = total

    others = pl.ds(0, (rows_n - 1) * chunk)

    def gather_start(s):
        mine = pl.ds(pl.multiple_of(me * chunk, chunk), chunk)
        for d in far:
            send(
                x_buf.at[s, mine], x_buf.at[s, mine], ag_s.at[s], ag_r.at[s], prow=row_peer(d)
            ).start()

    def top_start(s):
        for d in sorted(range(1, ny), key=lambda d: -min(d, ny - d)):
            piece = t_buf.at[s, y, x]
            send(
                piece, piece, ta_s.at[s], ta_r.at[s], prow=lax.rem(y + d, ny) * 2 + x
            ).start()

    def top_forward(s):
        arrived(t_buf.at[s, pl.ds(0, ny - 1), 0], ta_r.at[s])
        copy = send(
            t_buf.at[s, :, x], t_buf.at[s, :, x], tf_s.at[s], tf_r.at[s], prow=y * 2 + 1 - x
        )
        copy.start()
        return copy

    def scatter_copies(s):
        copies = []
        for m in sorted(range(1, rows_n), key=lambda m: -min(m, rows_n - m)):
            rows = pl.ds(m * chunk, chunk)
            src = (a_ref, d_top)[s].at[rows]
            dst = (t_buf.at[0, m // 2, m % 2], d_part)[s]
            copies.append(send(src, dst, sc_s.at[s], sc_r.at[s], prow=jnp.int32(m)))
        return copies

    def scatter_wait(s):
        piece = (t_buf.at[0, y, x], d_part)[s]

        @pl.when(jnp.logical_not(is_root))
        def _():
            arrived(piece, sc_r.at[s])

    reduce_start(0)
    top_panel_first()

    z1[...] = pick(source(col1))

    @pl.when(is_root)
    def _():
        wanted = source(sub + nb)
        onehot = (wanted == lane).astype(F32)
        moved = select(onehot.astype(BF16), a_ref[pl.ds(0, nb), :])
        swapped = jnp.max(onehot, axis=1, keepdims=True) > 0
        d_top[...] = jnp.where(swapped, moved, a_ref[pl.ds(nb, nb), :])
        d_part[...] = d_top[pl.ds(0, chunk), :]

    def tops(s):
        return t_buf[s].reshape(nb, -1)

    panel_x(0, lx0)

    reduce_finish(0)
    gather_start(0)

    @pl.when(is_root)
    def _():
        own_t.start()
        for copy in scatter_copies(0):
            copy.start()

    top_panel_x()
    lx1 = panel_start(1)

    panel_pass(0)

    @pl.when(is_root)
    def _():
        for copy in scatter_copies(1):
            copy.start()

    top_panel_z()
    def factor(s, b):
        per = nz * nxh // blocks
        return lf[s, pl.ds(b * per, per)].reshape(nb, nb)

    top_panel_core()
    panel_finish(0)

    scatter_wait(0)

    @pl.when(is_root)
    def _():
        own_t.wait()

    top_start(0)

    panel_own(1)
    panel_x(1, lx1)
    l_sel = None
    for b in range(blocks):
        onehot = (col1 == lane + (first + b * nb)).astype(F32).astype(BF16)
        part = select(onehot, factor(0, b))
        l_sel = part if l_sel is None else l_sel + part
    l_sel = split(l_sel)

    arrived(x_buf.at[0, others], ag_r.at[0])
    loads[2].wait()
    upper0 = matmul(linv_ref[0], x_buf[0])
    upper0_parts = split(upper0)
    rs_src[1] = (z1[...] - product(l_sel, upper0_parts)).reshape(rows_n, chunk, -1)
    reduce_start(1)

    top_panel_finish()
    scatter_wait(1)
    t_buf[1, y, x] = d_part[...] - product(split(lt[...]), upper0_parts)
    top_start(1)

    for b in range(blocks):
        rows = pl.ds(b * nb, nb)
        base[rows, :] = product(split(factor(0, b)), upper0_parts)

    panel_pass(1)

    reduce_finish(1)
    gather_start(1)
    tf0 = top_forward(0)
    tf1 = top_forward(1)

    panel_finish(1)

    tf0.wait_recv()
    for b in range(blocks):
        rows = pl.ds(b * nb, nb)
        hit = (sub + (first + b * nb) == row0).astype(F32)
        moved = select(hit.astype(BF16), tops(0))
        any_hit = jnp.max(hit, axis=1, keepdims=True) > 0
        base[rows, :] = jnp.where(any_hit, moved, a_ref[rows, :]) - base[rows, :]

    tf1.wait_recv()
    for b in range(blocks):
        rows = pl.ds(b * nb, nb)
        hit = (sub + (first + b * nb) == row1).astype(F32)
        moved = select(hit.astype(BF16), tops(1))
        any_hit = jnp.max(hit, axis=1, keepdims=True) > 0
        base[rows, :] = jnp.where(any_hit, moved, base[rows, :])

    arrived(x_buf.at[1, others], ag_r.at[1])
    upper1 = matmul(linv_ref[1], x_buf[1])
    upper1_parts = split(upper1)
    for b in range(blocks):
        rows = pl.ds(b * nb, nb)
        value = base[rows, :] - product(split(factor(1, b)), upper1_parts)
        if b == 0:
            value = jnp.where(is_root, upper0, value)
        if b == 1:
            value = jnp.where(is_root, upper1, value)
        out_ref[rows, :] = value

    for s in range(2):
        sent(lf.at[s, pl.ds(0, nxh - 1), 0], lx_s.at[s])
        sent(lf.at[s, pl.ds(0, (nz - 1) * nxh), 0], lz_s.at[s])
        sent(lf.at[s, :, 0], lc_s.at[s])
        sent(rs_src.at[s, pl.ds(1, rows_n - 1)], rs_s.at[s])
        sent(x_buf.at[s, others], ag_s.at[s])
        sent(t_buf.at[s, pl.ds(0, ny - 1), 0], ta_s.at[s])
    tf0.wait_send()
    tf1.wait_send()

    top_panel_sent()

    @pl.when(is_root)
    def _():
        for s in range(2):
            sent(d_top.at[others], sc_s.at[s])


def per_device(split, rows_n, matrix, l_panels, l_inverse, pivots):
    nz, nxh, nc = split
    rows_dev, cols_dev = matrix.shape
    nb = pivots.shape[1]
    chunk = nb // rows_n
    part = l_panels.shape[1]
    dma = pltpu.SemaphoreType.DMA
    vmem = pl.BlockSpec(memory_space=pltpu.VMEM)
    return pl.pallas_call(
        functools.partial(kernel, (rows_n, nz, nxh, nc, nb)),
        out_shape=jax.ShapeDtypeStruct(matrix.shape, F32),
        in_specs=[pl.BlockSpec(memory_space=pltpu.HBM)] * 4,
        out_specs=vmem,
        scratch_shapes=[
            pltpu.VMEM(matrix.shape, F32),
            pltpu.VMEM(l_inverse.shape, F32),
            pltpu.VMEM(pivots.shape, jnp.int32),
            pltpu.VMEM((2, rows_n, chunk, cols_dev), F32),
            pltpu.VMEM((2, rows_n, chunk, cols_dev), F32),
            pltpu.VMEM((2, nb, cols_dev), F32),
            pltpu.VMEM((2, rows_n // 2, 2, chunk, cols_dev), F32),
            pltpu.VMEM((nb, cols_dev), F32),
            pltpu.VMEM((chunk, cols_dev), F32),
            pltpu.VMEM((part, nb), F32),
            pltpu.VMEM((2, nz * nxh, nc, part, nb), F32),
            pltpu.VMEM((nb, cols_dev), F32),
            pltpu.VMEM((rows_dev, cols_dev), F32),
            dma((2,)), dma((2,)), dma((2,)), dma((2,)),
            dma((2,)), dma((2,)), dma((2,)), dma((2,)), dma((2,)), dma((2,)),
            dma((2,)), dma((2, nxh)), dma((2,)), dma((2, nxh + 4)), dma((2,)), dma((2,)),
            dma((4,)), dma((4,)),
            dma((3,)), dma((4,)),
        ],
        compiler_params=pltpu.CompilerParams(
            collective_id=0, has_side_effects=True, vmem_limit_bytes=VMEM_LIMIT
        ),
    )(*[
        pltpu.with_memory_space_constraint(v, pltpu.HBM)
        for v in (matrix, l_panels, l_inverse, pivots)
    ])


def solution(mesh):
    placed = (P("prow", "pcol"), P(None, ("prow", "pcol"), None), P(), P())
    body = functools.partial(per_device, split_cols(mesh), mesh.shape["prow"])
    return jax.shard_map(
        body, mesh=mesh, in_specs=placed, out_specs=P("prow", "pcol"), check_vma=False
    )
```
